256 devices in a mesh: slab: 128 (over x, z, y), pencil: 2 (over core).
Axes of the slice: x: 4, y: 4, z: 8, core: 2. Of those that a mesh axis runs over, the one named last changes fastest.
Arguments:
- density: float32 [768, 768, 384], P('slab', 'pencil'), may hold values from 0 to 1
- cell_kind: int32 [768, 768, 384], P('slab', 'pencil'), may hold values from 0 to 2
- sharpness: float32 [1], replicated, may hold values from 48 to 96
- fraction: float32 [1], replicated, may hold values from 0.36 to 0.41
Outputs:
- physical: float32 [768, 768, 384], P('slab', 'pencil')
- threshold: float32 [1], replicated
The draws below stay inside these ranges and needn't reach their ends.
Inputs may be any that keep to these rules, and one draw needn't show every extreme that they name: `cell_kind`: each cell is a design, void or solid cell.
All inputs are finite; a program needn't handle non-finite values.
Results may differ from the reference program's by a relative error of at most 0.0003.
Values sent between devices are 32-bit elements; how exact they have to be, the bound alone decides.
No kernel may reach another device: no remote copies, remote signals or barrier semaphores. Data moves between devices by JAX's collectives and lax.ppermute only.
A program may use at most 128 MiB of HBM per device.

```python
import math
import jax
import jax.numpy as jnp
from jax import lax

RADIUS = 5
ITERS = 3
NZ = 768
NY = 768
NX = 384


def draw_density(key, part):
    wave_draw = jax.random.uniform(jax.random.fold_in(key, 11), (6, 3), jnp.float32)
    sign_flip = jnp.where(jax.random.bernoulli(jax.random.fold_in(key, 12), 0.5, (6, 3)), 1.0, -1.0)
    phase_shift = jax.random.uniform(jax.random.fold_in(key, 13), (6,), jnp.float32, -math.pi, math.pi)
    cycles = sign_flip / (24.0 * jnp.power(4.0, wave_draw))
    depth_axis = jnp.arange(NZ, dtype=jnp.float32)[:, None, None]
    row_axis = jnp.arange(NY, dtype=jnp.float32)[None, :, None]
    column_axis = jnp.arange(NX, dtype=jnp.float32)[None, None, :]
    pattern = jnp.zeros((NZ, NY, NX), jnp.float32)
    for component in range(6):
        argument = cycles[component, 0] * depth_axis + cycles[component, 1] * row_axis + cycles[component, 2] * column_axis
        pattern = pattern + jnp.cos(2.0 * math.pi * argument + phase_shift[component])
    pattern = pattern / math.sqrt(3.0)
    middle_value = 0.62
    amplitude = 0.3
    roughness = 0.2
    jitter = jax.random.uniform(jax.random.fold_in(key, 14), (NZ, NY, NX), jnp.float32, -roughness, roughness)
    return jnp.clip(middle_value + amplitude * pattern + jitter, 0.0, 1.0).astype(jnp.float32)


def set_ends(result, stream_key, low, largest):
    dims = result.shape
    place = [jax.random.randint(jax.random.fold_in(stream_key, axis), (), 0, dims[axis]) for axis in range(len(dims))]
    result = result.at[tuple(place)].set(low)
    longest = dims.index(max(dims))
    place[longest] = (place[longest] + 1) % dims[longest]
    return result.at[tuple(place)].set(largest)


def setup_inputs(seed: int = 0) -> dict:
    key_list = jax.random.split(jax.random.key(seed), 5)
    density = draw_density(jax.random.fold_in(key_list[4], 71), 0)
    cell_kind = set_ends(jax.random.randint(key_list[1], (NZ, NY, NX), 0, 3), jax.random.fold_in(key_list[1], 1), 0, 2).astype(jnp.int32)
    sharpness = jnp.clip(jnp.exp(jax.random.uniform(key_list[2], (1,), jnp.float32, math.log(48.0), math.log(96.0))), 48.0, 96.0)
    fraction = jnp.clip(jax.random.uniform(key_list[3], (1,), jnp.float32, 0.36, 0.41), 0.36, 0.41)
    return dict(density=density, cell_kind=cell_kind, sharpness=sharpness, fraction=fraction)


def smooth_axis(field, axis):
    length = field.shape[axis]
    pads = [(0, 0), (0, 0), (0, 0)]
    pads[axis] = (RADIUS, RADIUS)
    padded = jnp.pad(field, pads)
    total = jnp.zeros_like(field)
    for offset in range(-RADIUS, RADIUS + 1):
        weight = float(RADIUS + 1 - abs(offset))
        piece = lax.slice_in_dim(padded, RADIUS + offset, RADIUS + offset + length, axis=axis)
        total = total + weight * piece
    return total


def coverage(count):
    index = jnp.arange(count, dtype=jnp.int32)
    total = jnp.zeros((count,), jnp.float32)
    for offset in range(-RADIUS, RADIUS + 1):
        inside = ((index + offset >= 0) & (index + offset < count)).astype(jnp.float32)
        total = total + float(RADIUS + 1 - abs(offset)) * inside
    return total


def project(filtered, cell_kind, beta, level):
    tangent = jnp.tanh(beta * (filtered - level))
    design = cell_kind == 0
    solid = cell_kind == 2
    values = jnp.where(design, 0.5 * (1.0 + tangent), jnp.where(solid, 1.0, 0.0))
    return values, tangent, design


def reference(density, cell_kind, sharpness, fraction):
    smoothed = smooth_axis(smooth_axis(smooth_axis(density, 0), 1), 2)
    cover = coverage(NZ)[:, None, None] * coverage(NY)[None, :, None] * coverage(NX)[None, None, :]
    filtered = smoothed / cover
    beta = sharpness[0]
    cells = jnp.float32(NZ * NY * NX)
    level = jnp.float32(0.5)
    for step in range(ITERS):
        values, tangent, design = project(filtered, cell_kind, beta, level)
        volume = jnp.sum(values)
        slope = cells + jnp.sum(jnp.where(design, 0.5 * beta * (1.0 - tangent * tangent), 0.0))
        level = level + (volume - fraction[0] * cells) / slope
    values, tangent, design = project(filtered, cell_kind, beta, level)
    return values, jnp.reshape(level, (1,)).astype(jnp.float32)
```

```python
import functools

import jax
import jax.numpy as jnp
from jax import lax
from jax.experimental import pallas as pl
from jax.experimental.pallas import tpu as pltpu

RADIUS = 5
ITERS = 3
REACH = 8
ROWS = 48
FAR = 1e30
LIMIT = 8 << 20
AHEAD = 2
DEVICES = ("slab", "pencil")


VMEM = pl.BlockSpec(memory_space=pltpu.VMEM)
SMEM = pl.BlockSpec(memory_space=pltpu.SMEM)


def call(kernel, name, outs, ins, out_specs, in_specs, scratch=(), flops=0, moved=0):
    return pl.pallas_call(
        kernel,
        name=name,
        out_shape=outs,
        in_specs=in_specs,
        out_specs=out_specs,
        scratch_shapes=list(scratch),
        compiler_params=pltpu.CompilerParams(vmem_limit_bytes=LIMIT),
        cost_estimate=pl.CostEstimate(flops=flops, bytes_accessed=moved, transcendentals=0),
    )(*ins)


def along_z(layers, depth):
    pairs = [a + b for a, b in zip(layers[:-1], layers[1:])]
    sixes = [pairs[i] + pairs[i + 2] + pairs[i + 4] for i in range(depth + RADIUS)]
    pairs = [a + b for a, b in zip(sixes[:-1], sixes[1:])]
    return [pairs[i] + pairs[i + 2] + pairs[i + 4] for i in range(depth)]


def parts(x):
    high = x.astype(jnp.bfloat16)
    return high, (x - high.astype(jnp.float32)).astype(jnp.bfloat16)


def zx_kernel(sends, density, below, above, weights, _, *refs):
    if sends:
        ahead, out, last, leading, high, low = refs
        last[...] = ahead[ahead.shape[0] - RADIUS :]
        leading[...] = ahead[:RADIUS]
    else:
        out, high, low = refs
    depth, rows, cols = out.shape
    for r in range(0, rows, 16):
        for c in range(0, cols, 128):
            at = (slice(r, r + 16), slice(c, c + 128))
            layers = [below[(i, *at)] for i in range(RADIUS)]
            layers += [density[(i, *at)] for i in range(depth)]
            layers += [above[(i, *at)] for i in range(RADIUS)]
            for i, value in enumerate(along_z(layers, depth)):
                high[(i, *at)], low[(i, *at)] = parts(value)
    flat = (depth * rows, cols)
    w = weights[...]
    total = jnp.dot(low[...].reshape(flat), w, preferred_element_type=jnp.float32)
    total += jnp.dot(high[...].reshape(flat), w, preferred_element_type=jnp.float32)
    out[...] = total.reshape(out.shape)


def zx(chunk, ahead, density, below, above, weights, after):
    depth, rows, cols = density.shape[0], ROWS, density.shape[2]
    sends = ahead is not None
    f32 = jnp.float32
    halo = pl.BlockSpec((RADIUS, rows, cols), lambda i: (0, 0, 0))
    whole = pl.BlockSpec((depth, rows, cols), lambda i: (0, 0, 0))
    part = lambda k: pl.BlockSpec((depth, rows, cols), lambda i: (0, k, 0))
    return pl.pallas_call(
        functools.partial(zx_kernel, sends),
        name=f"zx{chunk}",
        grid=(1,),
        out_shape=[jax.ShapeDtypeStruct((depth, rows, cols), f32)]
        + [jax.ShapeDtypeStruct((RADIUS, rows, cols), f32)] * (2 * sends),
        in_specs=[
            part(chunk),
            halo,
            halo,
            pl.BlockSpec((cols, cols), lambda i: (0, 0)),
            pl.BlockSpec(memory_space=pl.ANY),
            *([part(ahead)] * sends),
        ],
        out_specs=[whole] + [halo] * (2 * sends),
        scratch_shapes=[pltpu.VMEM((depth, rows, cols), jnp.bfloat16)] * 2,
        compiler_params=pltpu.CompilerParams(vmem_limit_bytes=LIMIT),
        cost_estimate=pl.CostEstimate(flops=4_000_000, bytes_accessed=2_000_000, transcendentals=0),
    )(density, below, above, weights, after, *([density] * sends))


def coverage(index, whole):
    total = jnp.zeros(index.shape, jnp.float32)
    for offset in range(-RADIUS, RADIUS + 1):
        inside = (index + offset >= 0) & (index + offset < whole)
        total = total + jnp.where(inside, float(RADIUS + 1 - abs(offset)), 0.0)
    return total


def tally(t):
    ones = 1.0 - t * t
    return t.reshape(-1, 8, t.shape[1]).sum(0), ones.reshape(-1, 8, t.shape[1]).sum(0)


def y_kernel(before_row, beta, before, here, after, kind, rz, scale, weights, field, sums, high):
    depth, rows, cols = here.shape
    w = weights[...]
    b = beta[0]
    both = jnp.zeros((2, 8, cols), jnp.float32)
    for i in range(depth):
        tall = jnp.concatenate(
            [before[i, before_row : before_row + REACH, :], here[i], after[i, :REACH, :]], axis=0
        )
        top, rest = parts(tall)
        stack = jnp.concatenate([top, rest], axis=0)
        smooth = jnp.dot(w, stack, preferred_element_type=jnp.float32)
        filtered = smooth * (scale[...] * rz[i])
        what = kind[i]
        value = jnp.where(what == 0, filtered, jnp.where(what == 2, FAR, -FAR))
        field[i] = value
        t = jnp.tanh(b * (value - 0.5))
        both += jnp.stack(tally(t))
    sums[...] = both


def y_pass(chunk, beta, before, here, after, kind, rz, scale, weights):
    depth, rows, cols = here.shape
    before_row = before.shape[1] - REACH
    shapes = [before.shape, here.shape, after.shape]
    whole = lambda s: pl.BlockSpec(s, lambda i: (0,) * len(s))
    return pl.pallas_call(
        functools.partial(y_kernel, before_row),
        name=f"y{chunk}",
        grid=(1,),
        out_shape=(
            jax.ShapeDtypeStruct((depth, rows, cols), jnp.float32),
            jax.ShapeDtypeStruct((2, 8, cols), jnp.float32),
        ),
        in_specs=[SMEM, *map(whole, shapes)]
        + [pl.BlockSpec((depth, rows, cols), lambda i: (0, chunk, 0)), SMEM]
        + [pl.BlockSpec((rows, cols), lambda i: (chunk, 0)), whole(weights.shape)],
        out_specs=(whole((depth, rows, cols)), whole((2, 8, cols))),
        scratch_shapes=[pltpu.VMEM((8, 128), jnp.float32)],
        compiler_params=pltpu.CompilerParams(vmem_limit_bytes=LIMIT),
        cost_estimate=pl.CostEstimate(flops=4_000_000, bytes_accessed=2_000_000, transcendentals=0),
    )(beta, before, here, after, kind, rz, scale, weights)


def pack(both, message):
    folded = both[:, :, 0:128] + both[:, :, 128:256] + both[:, :, 256:384]
    row = jnp.sum(folded, axis=1)
    row = row[:, 0:64] + row[:, 64:128]
    line = jnp.concatenate([row[0:1], row[1:2]], axis=1)
    message[...] = jnp.broadcast_to(line, message.shape)


def newton(cells, message, level, beta, fraction):
    line = jnp.sum(message[...], axis=0, keepdims=True)
    lane = lax.broadcasted_iota(jnp.int32, line.shape, 1)
    total = jnp.sum(jnp.where(lane < 64, line, 0.0))
    bends = jnp.sum(jnp.where(lane < 64, 0.0, line))
    volume = 0.5 * (cells + total)
    top = jnp.full((8, 128), volume - fraction[0] * cells, jnp.float32)
    bottom = jnp.full((8, 128), cells + 0.5 * beta[0] * bends, jnp.float32)
    return level + jnp.max(top / bottom)


def first_kernel(count, *refs):
    sums, message = refs[:count], refs[count]
    pack(functools.reduce(jnp.add, [s[...] for s in sums]), message)


def again_kernel(cells, count, message, level, beta, fraction, *refs):
    fields, (sent, moved) = refs[:count], refs[count:]
    eta = newton(cells, message, level[0], beta, fraction)
    moved[0] = eta
    b = beta[0]
    cols = fields[0].shape[2]
    both = jnp.zeros((2, 8, cols), jnp.float32)
    for field in fields:
        for i in range(field.shape[0]):
            both += jnp.stack(tally(jnp.tanh(b * (field[i] - eta))))
    pack(both, sent)


def last_kernel(cells, count, message, level, beta, fraction, *refs):
    fields, (out, moved, held, sems) = refs[:count], refs[count:]
    eta = newton(cells, message, level[0], beta, fraction)
    moved[0] = eta
    b = beta[0]
    copies = []
    for k, field in enumerate(fields):
        rows = pl.ds(k * field.shape[1], field.shape[1])
        for i in range(field.shape[0]):
            held[i, rows, :] = 0.5 * (1.0 + jnp.tanh(b * (field[i] - eta)))
        copies.append(pltpu.make_async_copy(held.at[:, rows, :], out.at[:, rows, :], sems.at[k]))
        copies[-1].start()
    for copy in copies:
        copy.wait()


def local(slabs, pencils, density, cell_kind, beta, fraction):
    depth, rows, cols = density.shape
    members = slabs * pencils
    cells = float(depth * slabs * rows * pencils * cols)
    count = rows // ROWS
    up = [(i, i + 1) for i in range(slabs - 1)]
    down = [(j, i) for i, j in up]

    near = lax.broadcasted_iota(jnp.int32, (cols, cols), 0)
    near = jnp.abs(near - lax.broadcasted_iota(jnp.int32, (cols, cols), 1))
    wx = jnp.maximum(RADIUS + 1 - near, 0).astype(jnp.bfloat16)
    tall = ROWS + 2 * REACH
    near = lax.broadcasted_iota(jnp.int32, (ROWS, 2 * tall), 1) % tall
    near = jnp.abs(near - REACH - lax.broadcasted_iota(jnp.int32, (ROWS, 2 * tall), 0))
    wy = jnp.maximum(RADIUS + 1 - near, 0).astype(jnp.bfloat16)
    rz = 1.0 / coverage(lax.axis_index("slab") * depth + jnp.arange(depth), depth * slabs)
    cy = coverage(lax.axis_index("pencil") * rows + jnp.arange(rows), rows * pencils)
    scale = 1.0 / (cy[:, None] * coverage(jnp.arange(cols), cols)[None, :])

    order = [count - 1, *range(count - 1)]
    side = [(i, i + 1) for i in range(pencils - 1)]
    smooth, fields, sums = {}, {}, {}
    arrived = []

    def send(last, leading):
        arrived.append((lax.ppermute(last, "slab", up), lax.ppermute(leading, "slab", down)))

    def y(k):
        fields[k], sums[k] = y_pass(
            k,
            beta,
            before if k == 0 else smooth[k - 1],
            smooth[k],
            after if k == count - 1 else smooth[k + 1],
            cell_kind,
            rz,
            scale,
            wy,
        )
        return sums[k]

    for k in order[:AHEAD]:
        at = slice(k * ROWS, (k + 1) * ROWS)
        send(density[depth - RADIUS :, at], density[:RADIUS, at])
    token = jnp.zeros((8, 128), jnp.float32)
    for n, k in enumerate(order):
        ahead = order[n + AHEAD] if n + AHEAD < count else None
        smooth[k], *sent = zx(k, ahead, density, *arrived[n], wx, token)
        if sent:
            send(*sent)
        if n == 0:
            before = lax.ppermute(smooth[k][:, ROWS - REACH :], "pencil", side)
        elif n == 1:
            after = lax.ppermute(smooth[0][:, :REACH], "pencil", [(j, i) for i, j in side])
        else:
            token = y(k - 1)
    y(count - 2)
    y(count - 1)
    fields, sums = ([d[k] for k in range(count)] for d in (fields, sums))

    f32 = jnp.float32
    sent = jax.ShapeDtypeStruct((members, 128), f32)
    one = jax.ShapeDtypeStruct((1,), f32)
    message = call(
        functools.partial(first_kernel, count), "first", sent, sums, VMEM, [VMEM] * count,
        flops=100_000, moved=200_000,
    )
    level = jnp.full((1,), 0.5, f32)
    scalars = [VMEM, SMEM, SMEM, SMEM]
    for step in range(ITERS):
        message = lax.all_to_all(message, DEVICES, 0, 0, tiled=True)
        ins = [message, level, beta, fraction, *fields]
        if step < ITERS - 1:
            message, level = call(
                functools.partial(again_kernel, cells, count), f"again{step}", (sent, one), ins,
                (VMEM, SMEM), scalars + [VMEM] * count, flops=6_000_000, moved=3_600_000,
            )
    physical, level = call(
        functools.partial(last_kernel, cells, count), "last",
        (jax.ShapeDtypeStruct(density.shape, f32), one), ins,
        (pl.BlockSpec(memory_space=pl.ANY), SMEM), scalars + [VMEM] * count,
        [pltpu.VMEM(density.shape, f32), pltpu.SemaphoreType.DMA((count,))],
        flops=6_000_000, moved=7_200_000,
    )
    return physical, level


def solution(mesh):
    P = jax.sharding.PartitionSpec
    grid = P("slab", "pencil", None)
    return jax.shard_map(
        functools.partial(local, mesh.shape["slab"], mesh.shape["pencil"]),
        mesh=mesh,
        in_specs=(grid, grid, P(), P()),
        out_specs=(grid, P()),
        check_vma=False,
    )
```

```python
import functools

import jax
import jax.numpy as jnp
from jax import lax
from jax.experimental import pallas as pl
from jax.experimental.pallas import tpu as pltpu

RADIUS = 5
ITERS = 3
REACH = 8
MOST = 112
FAR = 1e30
LIMIT = 16 << 20
SHARES = (192, 64)
DEVICES = ("slab", "pencil")


VMEM = pl.BlockSpec(memory_space=pltpu.VMEM)
SMEM = pl.BlockSpec(memory_space=pltpu.SMEM)


def call(kernel, name, outs, ins, out_specs, in_specs, scratch=(), flops=0, moved=0):
    return pl.pallas_call(
        kernel,
        name=name,
        out_shape=outs,
        in_specs=in_specs,
        out_specs=out_specs,
        scratch_shapes=list(scratch),
        compiler_params=pltpu.CompilerParams(vmem_limit_bytes=LIMIT),
        cost_estimate=pl.CostEstimate(flops=flops, bytes_accessed=moved, transcendentals=0),
    )(*ins)


def along_z(layers, depth):
    pairs = [a + b for a, b in zip(layers[:-1], layers[1:])]
    sixes = [pairs[i] + pairs[i + 2] + pairs[i + 4] for i in range(depth + RADIUS)]
    pairs = [a + b for a, b in zip(sixes[:-1], sixes[1:])]
    return [pairs[i] + pairs[i + 2] + pairs[i + 4] for i in range(depth)]


def parts(x):
    high = x.astype(jnp.bfloat16)
    return high, (x - high.astype(jnp.float32)).astype(jnp.bfloat16)


def filter_zx(density, start, below, above, weights, out, high, low):
    depth, rows, cols = out.shape
    for r in range(0, rows, 16):
        for c in range(0, cols, 128):
            at = (slice(r, r + 16), slice(c, c + 128))
            layers = [below[(i, *at)] for i in range(RADIUS)]
            layers += [density[i, start + r : start + r + 16, c : c + 128] for i in range(depth)]
            layers += [above[(i, *at)] for i in range(RADIUS)]
            for i, value in enumerate(along_z(layers, depth)):
                high[(i, *at)], low[(i, *at)] = parts(value)
    w = weights[...]
    for i in range(depth):
        total = jnp.dot(low[i], w, preferred_element_type=jnp.float32)
        out[i] = total + jnp.dot(high[i], w, preferred_element_type=jnp.float32)


def zx_kernel(start, edge, density, below, above, weights, _, out, side, high, low):
    filter_zx(density, start, below, above, weights, out, high, low)
    side[...] = out[:, edge : edge + REACH, :]


def zx(start, edge, density, below, above, weights, earlier):
    depth, cols = density.shape[0], density.shape[2]
    rows = below.shape[1]
    shape = lambda r: jax.ShapeDtypeStruct((depth, r, cols), jnp.float32)
    return call(
        functools.partial(zx_kernel, start, edge), f"zx{start}", (shape(rows), shape(REACH)),
        (density, below, above, weights, earlier), (VMEM, VMEM),
        [VMEM] * 4 + [pl.BlockSpec(memory_space=pl.ANY)],
        [pltpu.VMEM((depth, rows, cols), jnp.bfloat16)] * 2,
        flops=rows * 100_000, moved=rows * 40_000,
    )


def coverage(index, whole):
    total = jnp.zeros(index.shape, jnp.float32)
    for offset in range(-RADIUS, RADIUS + 1):
        inside = (index + offset >= 0) & (index + offset < whole)
        total = total + jnp.where(inside, float(RADIUS + 1 - abs(offset)), 0.0)
    return total


def tally(t):
    ones = 1.0 - t * t
    return t.reshape(-1, 8, t.shape[1]).sum(0), ones.reshape(-1, 8, t.shape[1]).sum(0)


def band(rows):
    tall = rows + 2 * REACH
    column = lax.broadcasted_iota(jnp.int32, (rows, 2 * tall), 1)
    column = jnp.where(column >= tall, column - tall, column)
    away = jnp.abs(column - REACH - lax.broadcasted_iota(jnp.int32, (rows, 2 * tall), 0))
    return jnp.maximum(RADIUS + 1 - away, 0).astype(jnp.float32).astype(jnp.bfloat16)


def filter_y(pieces, start, kind, rz, scale, beta, field):
    depth, rows, cols = field.shape
    blocks = -(-rows // MOST)
    size = -(-rows // (8 * blocks)) * 8
    both = jnp.zeros((2, 8, cols), jnp.float32)
    for at in range(0, rows, size):
        length = min(size, rows - at)
        w = band(length)
        here = slice(start + at, start + at + length)
        for i in range(depth):
            tall = pieces(i, at, length + 2 * REACH)
            top, rest = parts(tall)
            stack = jnp.concatenate([top, rest], axis=0)
            smooth = jnp.dot(w, stack, preferred_element_type=jnp.float32)
            filtered = smooth * (scale[here, :] * rz[i])
            what = kind[i, here, :]
            value = jnp.where(what == 0, filtered, jnp.where(what == 2, FAR, -FAR))
            field[i, at : at + length, :] = value
            both += jnp.stack(tally(jnp.tanh(beta * (value - 0.5))))
    return both


def joined(*refs):
    def pieces(i, at, length):
        found, first = [], 0
        for ref, low, high in refs:
            a, b = max(at, first), min(at + length, first + high - low)
            if a < b:
                found.append(ref[i, low + a - first : low + b - first, :])
            first += high - low
        return found[0] if len(found) == 1 else jnp.concatenate(found, axis=0)

    return pieces


def sides_kernel(starts, beta, _, before, a, b, after, kind, rz, scale, field_a, field_b, sums):
    one = joined((before, 0, REACH), (a, 0, a.shape[1]))
    both = filter_y(one, starts[0], kind, rz, scale, beta[0], field_a)
    one = joined((b, 0, b.shape[1]), (after, 0, REACH))
    sums[...] = both + filter_y(one, starts[1], kind, rz, scale, beta[0], field_b)


def middle_kernel(
    start, beta, density, below, above, weights, a, b, kind, rz, scale, sums,
    field, message, own, high, low,
):
    filter_zx(density, start, below, above, weights, own, high, low)
    one = joined((a, a.shape[1] - 2 * REACH, a.shape[1]), (own, 0, own.shape[1]), (b, 0, 2 * REACH))
    both = filter_y(one, start - REACH, kind, rz, scale, beta[0], field)
    pack(sums[...] + both, message)


def pack(both, message):
    folded = both[:, :, 0:128] + both[:, :, 128:256] + both[:, :, 256:384]
    row = jnp.sum(folded, axis=1)
    row = row[:, 0:64] + row[:, 64:128]
    line = jnp.concatenate([row[0:1], row[1:2]], axis=1)
    message[...] = jnp.broadcast_to(line, message.shape)


def newton(cells, message, level, beta, fraction):
    line = jnp.sum(message[...], axis=0, keepdims=True)
    lane = lax.broadcasted_iota(jnp.int32, line.shape, 1)
    total = jnp.sum(jnp.where(lane < 64, line, 0.0))
    bends = jnp.sum(jnp.where(lane < 64, 0.0, line))
    volume = 0.5 * (cells + total)
    top = jnp.full((8, 128), volume - fraction[0] * cells, jnp.float32)
    bottom = jnp.full((8, 128), cells + 0.5 * beta[0] * bends, jnp.float32)
    return level + jnp.max(top / bottom)


def again_kernel(cells, count, message, level, beta, fraction, *refs):
    fields, (sent, moved) = refs[:count], refs[count:]
    eta = newton(cells, message, level[0], beta, fraction)
    moved[0] = eta
    b = beta[0]
    cols = fields[0].shape[2]
    both = jnp.zeros((2, 8, cols), jnp.float32)
    for field in fields:
        for i in range(field.shape[0]):
            both += jnp.stack(tally(jnp.tanh(b * (field[i] - eta))))
    pack(both, sent)


def last_kernel(cells, count, message, level, beta, fraction, *refs):
    fields, (out, moved, held, sems) = refs[:count], refs[count:]
    eta = newton(cells, message, level[0], beta, fraction)
    moved[0] = eta
    b = beta[0]
    copies = []
    first = 0
    for k, field in enumerate(fields):
        rows = pl.ds(first, field.shape[1])
        first += field.shape[1]
        for i in range(field.shape[0]):
            held[i, rows, :] = 0.5 * (1.0 + jnp.tanh(b * (field[i] - eta)))
        copies.append(pltpu.make_async_copy(held.at[:, rows, :], out.at[:, rows, :], sems.at[k]))
        copies[-1].start()
    for copy in copies:
        copy.wait()


def local(slabs, pencils, density, cell_kind, beta, fraction):
    depth, rows, cols = density.shape
    members = slabs * pencils
    cells = float(depth * slabs * rows * pencils * cols)
    up = [(i, i + 1) for i in range(slabs - 1)]
    down = [(j, i) for i, j in up]
    side = [(i, i + 1) for i in range(pencils - 1)]
    f32 = jnp.float32

    def across(source, first, size):
        last = source[depth - RADIUS :, first : first + size]
        leading = source[:RADIUS, first : first + size]
        return lax.ppermute(last, "slab", up), lax.ppermute(leading, "slab", down)

    mid, end = SHARES[0], sum(SHARES)
    halo_a = across(density, 0, mid)
    later = lax.optimization_barrier(density)
    halo_b = across(later, end, rows - end)
    halo_c = across(later, mid, end - mid)

    near = lax.broadcasted_iota(jnp.int32, (cols, cols), 0)
    near = jnp.abs(near - lax.broadcasted_iota(jnp.int32, (cols, cols), 1))
    wx = jnp.maximum(RADIUS + 1 - near, 0).astype(jnp.bfloat16)
    rz = 1.0 / coverage(lax.axis_index("slab") * depth + jnp.arange(depth), depth * slabs)
    cy = coverage(lax.axis_index("pencil") * rows + jnp.arange(rows), rows * pencils)
    scale = 1.0 / (cy[:, None] * coverage(jnp.arange(cols), cols)[None, :])

    smooth_a, head = zx(0, 0, density, *halo_a, wx, beta)
    smooth_b, tail = zx(end, rows - end - REACH, density, *halo_b, wx, head)
    before = lax.ppermute(tail, "pencil", side)
    after = lax.ppermute(head, "pencil", [(j, i) for i, j in side])
    field = lambda n: jax.ShapeDtypeStruct((depth, n, cols), f32)
    sums = jax.ShapeDtypeStruct((2, 8, cols), f32)
    sent = jax.ShapeDtypeStruct((members, 128), f32)
    one = jax.ShapeDtypeStruct((1,), f32)
    inner = end - mid + 2 * REACH
    field_a, field_b, sums = call(
        functools.partial(sides_kernel, (0, end + REACH)), "sides",
        (field(mid - REACH), field(rows - end - REACH), sums),
        (beta, fraction, before, smooth_a, smooth_b, after, cell_kind, rz, scale),
        (VMEM,) * 3, [SMEM, SMEM, *[VMEM] * 5, SMEM, VMEM],
        flops=20_000_000, moved=10_000_000,
    )
    field_c, message = call(
        functools.partial(middle_kernel, mid), "middle", (field(inner), sent),
        (beta, density, *halo_c, wx, smooth_a, smooth_b, cell_kind, rz, scale, sums),
        (VMEM,) * 2, [SMEM, *[VMEM] * 7, SMEM, VMEM, VMEM],
        [pltpu.VMEM((depth, end - mid, cols), f32)]
        + [pltpu.VMEM((depth, end - mid, cols), jnp.bfloat16)] * 2,
        flops=6_000_000, moved=3_000_000,
    )
    fields = [field_a, field_c, field_b]
    count = len(fields)
    level = jnp.full((1,), 0.5, f32)
    scalars = [VMEM, SMEM, SMEM, SMEM]
    for step in range(ITERS):
        message = lax.all_to_all(message, DEVICES, 0, 0, tiled=True)
        ins = [message, level, beta, fraction, *fields]
        if step < ITERS - 1:
            message, level = call(
                functools.partial(again_kernel, cells, count), f"again{step}", (sent, one), ins,
                (VMEM, SMEM), scalars + [VMEM] * count, flops=6_000_000, moved=3_600_000,
            )
    return call(
        functools.partial(last_kernel, cells, count), "last", (field(rows), one), ins,
        (pl.BlockSpec(memory_space=pl.ANY), SMEM), scalars + [VMEM] * count,
        [pltpu.VMEM(density.shape, f32), pltpu.SemaphoreType.DMA((count,))],
        flops=6_000_000, moved=7_200_000,
    )


def solution(mesh):
    P = jax.sharding.PartitionSpec
    grid = P("slab", "pencil", None)
    return jax.shard_map(
        functools.partial(local, mesh.shape["slab"], mesh.shape["pencil"]),
        mesh=mesh,
        in_specs=(grid, grid, P(), P()),
        out_specs=(grid, P()),
        check_vma=False,
    )
```

```python
import functools

import jax
import jax.numpy as jnp
from jax import lax
from jax.experimental import pallas as pl
from jax.experimental.pallas import tpu as pltpu


RADIUS = 5
ITERS = 3
REACH = 8
MOST = 112
FAR = 1e30
LIMIT = 16 << 20
CHUNKS = ((320, 384), (0, 128), (176, 320), (128, 176))
DEVICES = ("slab", "pencil")


VMEM = pl.BlockSpec(memory_space=pltpu.VMEM)
SMEM = pl.BlockSpec(memory_space=pltpu.SMEM)


def call(kernel, outs, ins, out_specs, in_specs, scratch=(), flops=0, moved=0):
    return pl.pallas_call(
        kernel,
        out_shape=outs,
        in_specs=in_specs,
        out_specs=out_specs,
        scratch_shapes=list(scratch),
        compiler_params=pltpu.CompilerParams(vmem_limit_bytes=LIMIT),
        cost_estimate=pl.CostEstimate(flops=flops, bytes_accessed=moved, transcendentals=0),
    )(*ins)


def along_z(layers, depth):
    pairs = [a + b for a, b in zip(layers[:-1], layers[1:])]
    sixes = [pairs[i] + pairs[i + 2] + pairs[i + 4] for i in range(depth + RADIUS)]
    pairs = [a + b for a, b in zip(sixes[:-1], sixes[1:])]
    return [pairs[i] + pairs[i + 2] + pairs[i + 4] for i in range(depth)]


def parts(x):
    high = x.astype(jnp.bfloat16)
    return high, (x - high.astype(jnp.float32)).astype(jnp.bfloat16)


def filter_zx(density, start, below, above, weights, out, high, low):
    depth, rows, cols = out.shape
    for r in range(0, rows, 16):
        for c in range(0, cols, 128):
            at = (slice(r, r + 16), slice(c, c + 128))
            layers = [below[(i, *at)] for i in range(RADIUS)]
            layers += [density[i, start + r : start + r + 16, c : c + 128] for i in range(depth)]
            layers += [above[(i, *at)] for i in range(RADIUS)]
            for i, value in enumerate(along_z(layers, depth)):
                high[(i, *at)], low[(i, *at)] = parts(value)
    w = weights[...]
    for i in range(depth):
        total = jnp.dot(low[i], w, preferred_element_type=jnp.float32)
        out[i] = total + jnp.dot(high[i], w, preferred_element_type=jnp.float32)


def zx_kernel(chunks, density, weights, _, *refs):
    halos, (out, tail, head, high, low) = refs[: 2 * len(chunks)], refs[2 * len(chunks) :]
    first = 0
    for n, (start, end) in enumerate(chunks):
        rows = pl.ds(first, end - start)
        first += end - start
        own = [r.at[:, rows, :] for r in (out, high, low)]
        filter_zx(density, start, *halos[2 * n : 2 * n + 2], weights, *own)
    edge, turn = chunks[0][1] - chunks[0][0], first - (chunks[-1][1] - chunks[-1][0])
    tail[...] = out[:, edge - REACH : edge, :]
    head[...] = out[:, turn : turn + REACH, :]


def zx(chunks, density, halos, weights, earlier):
    depth, cols = density.shape[0], density.shape[2]
    rows = sum(end - start for start, end in chunks)
    shape = lambda r: jax.ShapeDtypeStruct((depth, r, cols), jnp.float32)
    return call(
        functools.partial(zx_kernel, chunks),
        (shape(rows), shape(REACH), shape(REACH)),
        (density, weights, earlier, *(h for pair in halos for h in pair)), (VMEM,) * 3,
        [VMEM, VMEM, pl.BlockSpec(memory_space=pl.ANY)] + [VMEM] * (2 * len(halos)),
        [pltpu.VMEM((depth, rows, cols), jnp.bfloat16)] * 2,
        flops=rows * 100_000, moved=rows * 40_000,
    )


def coverage(index, whole):
    total = jnp.zeros(index.shape, jnp.float32)
    for offset in range(-RADIUS, RADIUS + 1):
        inside = (index + offset >= 0) & (index + offset < whole)
        total = total + jnp.where(inside, float(RADIUS + 1 - abs(offset)), 0.0)
    return total


def tally(t):
    ones = 1.0 - t * t
    return t.reshape(-1, 8, t.shape[1]).sum(0), ones.reshape(-1, 8, t.shape[1]).sum(0)


def band(rows):
    tall = rows + 2 * REACH
    column = lax.broadcasted_iota(jnp.int32, (rows, 2 * tall), 1)
    column = jnp.where(column >= tall, column - tall, column)
    away = jnp.abs(column - REACH - lax.broadcasted_iota(jnp.int32, (rows, 2 * tall), 0))
    return jnp.maximum(RADIUS + 1 - away, 0).astype(jnp.float32).astype(jnp.bfloat16)


def filter_y(pieces, start, kind, rz, scale, beta, field):
    depth, rows, cols = field.shape
    blocks = -(-rows // MOST)
    size = -(-rows // (8 * blocks)) * 8
    both = jnp.zeros((2, 8, cols), jnp.float32)
    for at in range(0, rows, size):
        length = min(size, rows - at)
        w = band(length)
        here = slice(start + at, start + at + length)
        for i in range(depth):
            tall = pieces(i, at, length + 2 * REACH)
            top, rest = parts(tall)
            stack = jnp.concatenate([top, rest], axis=0)
            smooth = jnp.dot(w, stack, preferred_element_type=jnp.float32)
            filtered = smooth * (scale[here, :] * rz[i])
            what = kind[i, here, :]
            value = jnp.where(what == 0, filtered, jnp.where(what == 2, FAR, -FAR))
            field[i, at : at + length, :] = value
            both += jnp.stack(tally(jnp.tanh(beta * (value - 0.5))))
    return both


def joined(*refs):
    def pieces(i, at, length):
        found, first = [], 0
        for ref, low, high in refs:
            a, b = max(at, first), min(at + length, first + high - low)
            if a < b:
                found.append(ref[i, low + a - first : low + b - first, :])
            first += high - low
        return found[0] if len(found) == 1 else jnp.concatenate(found, axis=0)

    return pieces


def sides_kernel(
    chunks, beta, _, before, a, b, after, kind, rz, scale, field_a, field_b, sums
):
    edge = chunks[0][1] - chunks[0][0]
    one = joined((before, 0, REACH), (a, edge, a.shape[1]))
    both = filter_y(one, 0, kind, rz, scale, beta[0], field_a)
    one = joined((b, 0, b.shape[1]), (a, 0, edge), (after, 0, REACH))
    start = chunks[2][0] + REACH
    sums[...] = both + filter_y(one, start, kind, rz, scale, beta[0], field_b)


def middle_kernel(
    start, beta, density, below, above, weights, a, b, kind, rz, scale, sums,
    field, message, own, high, low,
):
    filter_zx(density, start, below, above, weights, own, high, low)
    one = joined((a, a.shape[1] - 2 * REACH, a.shape[1]), (own, 0, own.shape[1]), (b, 0, 2 * REACH))
    both = filter_y(one, start - REACH, kind, rz, scale, beta[0], field)
    pack(sums[...] + both, message)


def pack(both, message):
    folded = both[:, :, 0:128] + both[:, :, 128:256] + both[:, :, 256:384]
    row = jnp.sum(folded, axis=1)
    row = row[:, 0:64] + row[:, 64:128]
    line = jnp.concatenate([row[0:1], row[1:2]], axis=1)
    message[...] = jnp.broadcast_to(line, message.shape)


def newton(cells, message, level, beta, fraction):
    line = jnp.sum(message[...], axis=0, keepdims=True)
    lane = lax.broadcasted_iota(jnp.int32, line.shape, 1)
    total = jnp.sum(jnp.where(lane < 64, line, 0.0), axis=1, keepdims=True)
    bends = jnp.sum(jnp.where(lane < 64, 0.0, line), axis=1, keepdims=True)
    volume = 0.5 * (cells + total)
    step = (volume - fraction[0] * cells) / (cells + 0.5 * beta[0] * bends)
    return level[...] + jnp.broadcast_to(step, level.shape)


def again_kernel(cells, count, message, level, beta, fraction, *refs):
    fields, (sent, moved) = refs[:count], refs[count:]
    eta = newton(cells, message, level, beta, fraction)
    moved[...] = eta
    b = beta[0]
    cols = fields[0].shape[2]
    eta = jnp.tile(eta[:1], (1, cols // 128))
    both = jnp.zeros((2, 8, cols), jnp.float32)
    for field in fields:
        for i in range(field.shape[0]):
            both += jnp.stack(tally(jnp.tanh(b * (field[i] - eta))))
    pack(both, sent)


def last_kernel(cells, count, message, level, beta, fraction, *refs):
    fields, (out, moved, held, sems) = refs[:count], refs[count:]
    eta = newton(cells, message, level, beta, fraction)
    moved[0] = eta[0, 0]
    b = beta[0]
    eta = jnp.tile(eta[:1], (1, held.shape[2] // 128))
    copies = []
    for i in range(held.shape[0]):
        first = 0
        for k, field in enumerate(fields):
            rows = pl.ds(first, field.shape[1])
            first += field.shape[1]
            held[i, rows, :] = 0.5 * (1.0 + jnp.tanh(b * (field[i] - eta)))
            at = (i, rows, slice(None))
            copies.append(pltpu.make_async_copy(held.at[at], out.at[at], sems.at[i * count + k]))
            copies[-1].start()
    for copy in copies:
        copy.wait()


def local(slabs, pencils, density, cell_kind, beta, fraction):
    depth, rows, cols = density.shape
    members = slabs * pencils
    cells = float(depth * slabs * rows * pencils * cols)
    up = [(i, i + 1) for i in range(slabs - 1)]
    down = [(j, i) for i, j in up]
    side = [(i, i + 1) for i in range(pencils - 1)]
    f32 = jnp.float32

    halos = []
    source = density
    for n, (start, end) in enumerate(CHUNKS):
        last, leading = source[depth - RADIUS :, start:end], source[:RADIUS, start:end]
        below = lax.ppermute(last, "slab", up)
        above = lax.ppermute(leading, "slab", down)
        halos.append((below, above))
        if n == 0:
            source = lax.optimization_barrier(density)

    near = lax.broadcasted_iota(jnp.int32, (cols, cols), 0)
    near = jnp.abs(near - lax.broadcasted_iota(jnp.int32, (cols, cols), 1))
    wx = jnp.maximum(RADIUS + 1 - near, 0).astype(jnp.bfloat16)
    rz = 1.0 / coverage(lax.axis_index("slab") * depth + jnp.arange(depth), depth * slabs)
    cy = coverage(lax.axis_index("pencil") * rows + jnp.arange(rows), rows * pencils)
    scale = 1.0 / (cy[:, None] * coverage(jnp.arange(cols), cols)[None, :])

    smooth_a, tail, head = zx(CHUNKS[:2], density, halos[:2], wx, beta)
    smooth_b, _, _ = zx(CHUNKS[2:3], density, halos[2:3], wx, head)
    before = lax.ppermute(tail, "pencil", side)
    after = lax.ppermute(head, "pencil", [(j, i) for i, j in side])
    field = lambda n: jax.ShapeDtypeStruct((depth, n, cols), f32)
    sums = jax.ShapeDtypeStruct((2, 8, cols), f32)
    sent = jax.ShapeDtypeStruct((members, 128), f32)
    one = jax.ShapeDtypeStruct((1,), f32)
    mid, end = CHUNKS[3]
    field_a, field_b, sums = call(
        functools.partial(sides_kernel, CHUNKS),
        (field(mid - REACH), field(rows - end - REACH), sums),
        (beta, fraction, before, smooth_a, smooth_b, after, cell_kind, rz, scale),
        (VMEM,) * 3, [SMEM, SMEM, *[VMEM] * 5, SMEM, VMEM],
        flops=20_000_000, moved=10_000_000,
    )
    field_c, message = call(
        functools.partial(middle_kernel, mid), (field(end - mid + 2 * REACH), sent),
        (beta, density, *halos[3], wx, smooth_a, smooth_b, cell_kind, rz, scale, sums),
        (VMEM,) * 2, [SMEM, *[VMEM] * 7, SMEM, VMEM, VMEM],
        [pltpu.VMEM((depth, end - mid, cols), f32)]
        + [pltpu.VMEM((depth, end - mid, cols), jnp.bfloat16)] * 2,
        flops=6_000_000, moved=3_000_000,
    )
    fields = [field_a, field_c, field_b]
    count = len(fields)
    level = jnp.full((8, 128), 0.5, f32)
    scalars = [VMEM, VMEM, SMEM, SMEM]
    for step in range(ITERS):
        message = lax.all_to_all(message, DEVICES, 0, 0, tiled=True)
        ins = [message, level, beta, fraction, *fields]
        if step < ITERS - 1:
            message, level = call(
                functools.partial(again_kernel, cells, count),
                (sent, jax.ShapeDtypeStruct(level.shape, f32)), ins,
                (VMEM, VMEM), scalars + [VMEM] * count, flops=6_000_000, moved=3_600_000,
            )
    return call(
        functools.partial(last_kernel, cells, count), (field(rows), one), ins,
        (pl.BlockSpec(memory_space=pl.ANY), SMEM), scalars + [VMEM] * count,
        [pltpu.VMEM(density.shape, f32), pltpu.SemaphoreType.DMA((count * depth,))],
        flops=6_000_000, moved=7_200_000,
    )


def solution(mesh):
    P = jax.sharding.PartitionSpec
    grid = P("slab", "pencil", None)
    return jax.shard_map(
        functools.partial(local, mesh.shape["slab"], mesh.shape["pencil"]),
        mesh=mesh,
        in_specs=(grid, grid, P(), P()),
        out_specs=(grid, P()),
        check_vma=False,
    )
```

```python
import functools

import jax
import jax.numpy as jnp
from jax import lax
from jax.experimental import pallas as pl
from jax.experimental.pallas import tpu as pltpu


RADIUS = 5
ITERS = 3
REACH = 8
MOST = 112
FAR = 1e30
LIMIT = 16 << 20
CHUNKS = ((288, 384), (0, 112), (144, 288), (112, 144))
PIECE = 32
DEVICES = ("slab", "pencil")


VMEM = pl.BlockSpec(memory_space=pltpu.VMEM)
SMEM = pl.BlockSpec(memory_space=pltpu.SMEM)


def call(kernel, outs, ins, out_specs, in_specs, scratch=(), flops=0, moved=0):
    return pl.pallas_call(
        kernel,
        out_shape=outs,
        in_specs=in_specs,
        out_specs=out_specs,
        scratch_shapes=list(scratch),
        compiler_params=pltpu.CompilerParams(vmem_limit_bytes=LIMIT),
        cost_estimate=pl.CostEstimate(flops=flops, bytes_accessed=moved, transcendentals=0),
    )(*ins)


def along_z(layers, depth):
    pairs = [a + b for a, b in zip(layers[:-1], layers[1:])]
    sixes = [pairs[i] + pairs[i + 2] + pairs[i + 4] for i in range(depth + RADIUS)]
    pairs = [a + b for a, b in zip(sixes[:-1], sixes[1:])]
    return [pairs[i] + pairs[i + 2] + pairs[i + 4] for i in range(depth)]


def parts(x):
    high = x.astype(jnp.bfloat16)
    return high, (x - high.astype(jnp.float32)).astype(jnp.bfloat16)


class Halo:
    def __init__(self, even, odd, held, sems, first, sem):
        rows = even.shape[1]
        self.held, self.first, self.copies = held, first, []
        for r in range(0, rows, PIECE):
            n = min(PIECE, rows - r)
            pair = []
            for k, ref in enumerate((even, odd)):
                here = held.at[k, :, pl.ds(first + r, n), :]
                pair.append(pltpu.make_async_copy(ref.at[:, pl.ds(r, n), :], here, sems.at[sem, k]))
                pair[-1].start()
            self.copies.append(pair)
            sem += 1
        self.sem = sem

    def wait(self, r):
        if r % PIECE == 0:
            for copy in self.copies[r // PIECE]:
                copy.wait()

    def layer(self, k, i, r, c):
        r += self.first
        return self.held[k, i, r : r + 16, c : c + 128]


def filter_zx(density, chunks, halos, parity, weights, out, high, low):
    depth, _, cols = out.shape
    odd = parity[0] == 1
    first = 0
    for (start, end), halo in zip(chunks, halos):
        for r in range(0, end - start, 16):
            halo.wait(r)
            for c in range(0, cols, 128):
                pairs = [[halo.layer(k, i, r, c) for k in (0, 1)] for i in range(RADIUS)]
                layers = [jnp.where(odd, e, o) for e, o in pairs]
                layers += [
                    density[i, start + r : start + r + 16, c : c + 128] for i in range(depth)
                ]
                layers += [jnp.where(odd, o, e) for e, o in pairs]
                at = (slice(first + r, first + r + 16), slice(c, c + 128))
                for i, value in enumerate(along_z(layers, depth)):
                    high[(i, *at)], low[(i, *at)] = parts(value)
        first += end - start
    w = weights[...]
    for i in range(depth):
        total = jnp.dot(low[i], w, preferred_element_type=jnp.float32)
        out[i] = total + jnp.dot(high[i], w, preferred_element_type=jnp.float32)


def scratch_zx(depth, cols, chunks):
    rows = sum(end - start for start, end in chunks)
    pieces = sum(-(-(end - start) // PIECE) for start, end in chunks)
    return [
        *[pltpu.VMEM((depth, rows, cols), jnp.bfloat16)] * 2,
        pltpu.VMEM((2, RADIUS, rows, cols), jnp.float32),
        pltpu.SemaphoreType.DMA((pieces, 2)),
    ]


def fetch(chunks, refs, held, sems):
    halos, first, sem = [], 0, 0
    for n, (start, end) in enumerate(chunks):
        halos.append(Halo(refs[2 * n], refs[2 * n + 1], held, sems, first, sem))
        first, sem = first + end - start, halos[-1].sem
    return halos


def zx_kernel(chunks, parity, density, weights, *refs):
    refs, (out, tail, head, high, low, held, sems) = refs[:-7], refs[-7:]
    halos = fetch(chunks, refs, held, sems)
    filter_zx(density, chunks, halos, parity, weights, out, high, low)
    edge = chunks[0][1] - chunks[0][0]
    tail[...] = out[:, edge - REACH : edge, :]
    head[...] = out[:, edge : edge + REACH, :]


def coverage(index, whole):
    total = jnp.zeros(index.shape, jnp.float32)
    for offset in range(-RADIUS, RADIUS + 1):
        inside = (index + offset >= 0) & (index + offset < whole)
        total = total + jnp.where(inside, float(RADIUS + 1 - abs(offset)), 0.0)
    return total


def tally(t):
    ones = 1.0 - t * t
    return t.reshape(-1, 8, t.shape[1]).sum(0), ones.reshape(-1, 8, t.shape[1]).sum(0)


def band(rows):
    tall = rows + 2 * REACH
    column = lax.broadcasted_iota(jnp.int32, (rows, 2 * tall), 1)
    column = jnp.where(column >= tall, column - tall, column)
    away = jnp.abs(column - REACH - lax.broadcasted_iota(jnp.int32, (rows, 2 * tall), 0))
    return jnp.maximum(RADIUS + 1 - away, 0).astype(jnp.float32).astype(jnp.bfloat16)


def filter_y(pieces, start, kind, rz, scale, beta, field):
    depth, rows, cols = field.shape
    blocks = -(-rows // MOST)
    size = -(-rows // (8 * blocks)) * 8
    both = jnp.zeros((2, 8, cols), jnp.float32)
    for at in range(0, rows, size):
        length = min(size, rows - at)
        w = band(length)
        here = slice(start + at, start + at + length)
        for i in range(depth):
            tall = pieces(i, at, length + 2 * REACH)
            top, rest = parts(tall)
            stack = jnp.concatenate([top, rest], axis=0)
            smooth = jnp.dot(w, stack, preferred_element_type=jnp.float32)
            filtered = smooth * (scale[here, :] * rz[i])
            what = kind[i, here, :]
            value = jnp.where(what == 0, filtered, jnp.where(what == 2, FAR, -FAR))
            field[i, at : at + length, :] = value
            both += jnp.stack(tally(jnp.tanh(beta * (value - 0.5))))
    return both


def joined(*refs):
    def pieces(i, at, length):
        found, first = [], 0
        for ref, low, high in refs:
            a, b = max(at, first), min(at + length, first + high - low)
            if a < b:
                found.append(ref[i, low + a - first : low + b - first, :])
            first += high - low
        return found[0] if len(found) == 1 else jnp.concatenate(found, axis=0)

    return pieces


def left_kernel(edge, beta, _, before, a, kind, rz, scale, field, sums):
    one = joined((before, 0, REACH), (a, edge, a.shape[1]))
    sums[...] = filter_y(one, 0, kind, rz, scale, beta[0], field)


def right_kernel(
    edge, chunk, parity, beta, density, even, odd, weights, a, after, kind, rz, scale, sums,
    own, field, more, high, low, held, sems,
):
    halos = fetch((chunk,), (even, odd), held, sems)
    filter_zx(density, (chunk,), halos, parity, weights, own, high, low)
    one = joined((own, 0, own.shape[1]), (a, 0, edge), (after, 0, REACH))
    more[...] = sums[...] + filter_y(one, chunk[0] + REACH, kind, rz, scale, beta[0], field)


def middle_kernel(
    chunk, parity, beta, density, even, odd, weights, a, b, kind, rz, scale, sums,
    field, message, own, high, low, held, sems,
):
    halos = fetch((chunk,), (even, odd), held, sems)
    filter_zx(density, (chunk,), halos, parity, weights, own, high, low)
    one = joined((a, a.shape[1] - 2 * REACH, a.shape[1]), (own, 0, own.shape[1]), (b, 0, 2 * REACH))
    both = filter_y(one, chunk[0] - REACH, kind, rz, scale, beta[0], field)
    pack(sums[...] + both, message)


def pack(both, message):
    folded = both[:, :, 0:128] + both[:, :, 128:256] + both[:, :, 256:384]
    row = jnp.sum(folded, axis=1)
    row = row[:, 0:64] + row[:, 64:128]
    line = jnp.concatenate([row[0:1], row[1:2]], axis=1)
    message[...] = jnp.broadcast_to(line, message.shape)


def newton(cells, message, level, beta, fraction):
    line = jnp.sum(message[...], axis=0, keepdims=True)
    lane = lax.broadcasted_iota(jnp.int32, line.shape, 1)
    total = jnp.sum(jnp.where(lane < 64, line, 0.0), axis=1, keepdims=True)
    bends = jnp.sum(jnp.where(lane < 64, 0.0, line), axis=1, keepdims=True)
    volume = 0.5 * (cells + total)
    step = (volume - fraction[0] * cells) / (cells + 0.5 * beta[0] * bends)
    return level[...] + jnp.broadcast_to(step, level.shape)


def again_kernel(cells, count, message, level, beta, fraction, *refs):
    fields, (sent, moved) = refs[:count], refs[count:]
    eta = newton(cells, message, level, beta, fraction)
    moved[...] = eta
    b = beta[0]
    cols = fields[0].shape[2]
    eta = jnp.tile(eta[:1], (1, cols // 128))
    both = jnp.zeros((2, 8, cols), jnp.float32)
    for field in fields:
        for i in range(field.shape[0]):
            both += jnp.stack(tally(jnp.tanh(b * (field[i] - eta))))
    pack(both, sent)


def last_kernel(cells, count, message, level, beta, fraction, *refs):
    fields, (out, moved, held, sems) = refs[:count], refs[count:]
    eta = newton(cells, message, level, beta, fraction)
    moved[0] = eta[0, 0]
    b = beta[0]
    eta = jnp.tile(eta[:1], (1, held.shape[2] // 128))
    copies = []
    for i in range(held.shape[0]):
        first = 0
        for k, field in enumerate(fields):
            rows = pl.ds(first, field.shape[1])
            first += field.shape[1]
            held[i, rows, :] = 0.5 * (1.0 + jnp.tanh(b * (field[i] - eta)))
            at = (i, rows, slice(None))
            copies.append(pltpu.make_async_copy(held.at[at], out.at[at], sems.at[i * count + k]))
            copies[-1].start()
    for copy in copies:
        copy.wait()


def local(slabs, pencils, density, cell_kind, beta, fraction):
    depth, rows, cols = density.shape
    members = slabs * pencils
    cells = float(depth * slabs * rows * pencils * cols)
    pairs = [
        [(a, b) for i in range(k, slabs - 1, 2) for a, b in ((i, i + 1), (i + 1, i))]
        for k in (0, 1)
    ]
    parity = lax.axis_index("slab") % 2
    side = [(i, i + 1) for i in range(pencils - 1)]
    f32 = jnp.float32

    halos = []
    source = density
    for n, (start, end) in enumerate(CHUNKS):
        for k in (0, 1):
            first = jnp.where(parity == k, depth - RADIUS, 0)
            part = lax.dynamic_slice_in_dim(source[:, start:end], first, RADIUS, axis=0)
            halos.append(lax.ppermute(part, "slab", pairs[k]))
        if n == 0:
            source = lax.optimization_barrier(density)
    parity = jnp.reshape(parity, (1,)).astype(jnp.int32)

    near = lax.broadcasted_iota(jnp.int32, (cols, cols), 0)
    near = jnp.abs(near - lax.broadcasted_iota(jnp.int32, (cols, cols), 1))
    wx = jnp.maximum(RADIUS + 1 - near, 0).astype(jnp.bfloat16)
    rz = 1.0 / coverage(lax.axis_index("slab") * depth + jnp.arange(depth), depth * slabs)
    cy = coverage(lax.axis_index("pencil") * rows + jnp.arange(rows), rows * pencils)
    scale = 1.0 / (cy[:, None] * coverage(jnp.arange(cols), cols)[None, :])

    field = lambda n: jax.ShapeDtypeStruct((depth, n, cols), f32)
    sums = jax.ShapeDtypeStruct((2, 8, cols), f32)
    sent = jax.ShapeDtypeStruct((members, 128), f32)
    one = jax.ShapeDtypeStruct((1,), f32)
    anywhere = pl.BlockSpec(memory_space=pl.ANY)
    size_a = sum(end - start for start, end in CHUNKS[:2])
    edge = CHUNKS[0][1] - CHUNKS[0][0]
    mid, end = CHUNKS[3]
    smooth_a, tail, head = call(
        functools.partial(zx_kernel, CHUNKS[:2]), (field(size_a), field(REACH), field(REACH)),
        (parity, density, wx, *halos[:4]), (VMEM,) * 3, [SMEM, VMEM, VMEM, *[anywhere] * 4],
        scratch_zx(depth, cols, CHUNKS[:2]), flops=20_000_000, moved=8_000_000,
    )
    before = lax.ppermute(tail, "pencil", side)
    after = lax.ppermute(head, "pencil", [(j, i) for i, j in side])
    field_a, sums_a = call(
        functools.partial(left_kernel, edge), (field(mid - REACH), sums),
        (beta, fraction, before, smooth_a, cell_kind, rz, scale),
        (VMEM,) * 2, [SMEM, SMEM, *[VMEM] * 3, SMEM, VMEM], flops=10_000_000, moved=4_000_000,
    )
    smooth_b, field_b, sums_b = call(
        functools.partial(right_kernel, edge, CHUNKS[2]),
        (field(CHUNKS[2][1] - end), field(rows - end - REACH), sums),
        (parity, beta, density, *halos[4:6], wx, smooth_a, after, cell_kind, rz, scale, sums_a),
        (VMEM,) * 3,
        [SMEM, SMEM, VMEM, anywhere, anywhere, *[VMEM] * 4, SMEM, VMEM, VMEM],
        scratch_zx(depth, cols, CHUNKS[2:3]), flops=20_000_000, moved=8_000_000,
    )
    field_c, message = call(
        functools.partial(middle_kernel, CHUNKS[3]),
        (field(end - mid + 2 * REACH), sent),
        (parity, beta, density, *halos[6:], wx, smooth_a, smooth_b, cell_kind, rz, scale, sums_b),
        (VMEM,) * 2, [SMEM, SMEM, VMEM, anywhere, anywhere, *[VMEM] * 4, SMEM, VMEM, VMEM],
        [pltpu.VMEM((depth, end - mid, cols), f32), *scratch_zx(depth, cols, CHUNKS[3:])],
        flops=6_000_000, moved=3_000_000,
    )
    fields = [field_a, field_c, field_b]
    count = len(fields)
    level = jnp.full((8, 128), 0.5, f32)
    scalars = [VMEM, VMEM, SMEM, SMEM]
    for step in range(ITERS):
        message = lax.all_to_all(message, DEVICES, 0, 0, tiled=True)
        ins = [message, level, beta, fraction, *fields]
        if step < ITERS - 1:
            message, level = call(
                functools.partial(again_kernel, cells, count),
                (sent, jax.ShapeDtypeStruct(level.shape, f32)), ins,
                (VMEM, VMEM), scalars + [VMEM] * count, flops=6_000_000, moved=3_600_000,
            )
    return call(
        functools.partial(last_kernel, cells, count), (field(rows), one), ins,
        (pl.BlockSpec(memory_space=pl.ANY), SMEM), scalars + [VMEM] * count,
        [pltpu.VMEM(density.shape, f32), pltpu.SemaphoreType.DMA((count * depth,))],
        flops=6_000_000, moved=7_200_000,
    )


def solution(mesh):
    P = jax.sharding.PartitionSpec
    grid = P("slab", "pencil", None)
    return jax.shard_map(
        functools.partial(local, mesh.shape["slab"], mesh.shape["pencil"]),
        mesh=mesh,
        in_specs=(grid, grid, P(), P()),
        out_specs=(grid, P()),
        check_vma=False,
    )
```

```python
import functools

import jax
import jax.numpy as jnp
from jax import lax
from jax.experimental import pallas as pl
from jax.experimental.pallas import tpu as pltpu


RADIUS = 5
ITERS = 3
REACH = 8
MOST = 112
FAR = 1e30
LIMIT = 16 << 20
CHUNKS = ((352, 384), (0, 176), (208, 352), (176, 208))
PIECE = 32
DEVICES = ("slab", "pencil")


VMEM = pl.BlockSpec(memory_space=pltpu.VMEM)
SMEM = pl.BlockSpec(memory_space=pltpu.SMEM)


def call(kernel, outs, ins, out_specs, in_specs, scratch=(), flops=0, moved=0):
    return pl.pallas_call(
        kernel,
        out_shape=outs,
        in_specs=in_specs,
        out_specs=out_specs,
        scratch_shapes=list(scratch),
        compiler_params=pltpu.CompilerParams(vmem_limit_bytes=LIMIT),
        cost_estimate=pl.CostEstimate(flops=flops, bytes_accessed=moved, transcendentals=0),
    )(*ins)


def along_z(layers, depth):
    pairs = [a + b for a, b in zip(layers[:-1], layers[1:])]
    sixes = [pairs[i] + pairs[i + 2] + pairs[i + 4] for i in range(depth + RADIUS)]
    pairs = [a + b for a, b in zip(sixes[:-1], sixes[1:])]
    return [pairs[i] + pairs[i + 2] + pairs[i + 4] for i in range(depth)]


def parts(x):
    high = x.astype(jnp.bfloat16)
    return high, (x - high.astype(jnp.float32)).astype(jnp.bfloat16)


class Halo:
    def __init__(self, even, odd, held, sems, first, sem):
        rows = even.shape[1]
        self.first, self.copies = first, []
        self.refs = [held.at[k] for k in (0, 1)]
        for r in range(0, rows, PIECE):
            n = min(PIECE, rows - r)
            pair = []
            for k, ref in enumerate((even, odd)):
                here = held.at[k, :, pl.ds(first + r, n), :]
                pair.append(pltpu.make_async_copy(ref.at[:, pl.ds(r, n), :], here, sems.at[sem, k]))
                pair[-1].start()
            self.copies.append(pair)
            sem += 1
        self.sem = sem

    def wait(self, r):
        if r % PIECE == 0:
            for copy in self.copies[r // PIECE]:
                copy.wait()


class Near:
    def __init__(self, even, odd):
        self.first, self.refs = 0, [even, odd]

    def wait(self, r):
        pass


def filter_zx(density, chunks, halos, place, weights, out, halves):
    depth, rows, cols = out.shape
    odd, edge = place[0] == 1, place[1] == 1
    first = 0
    for (start, end), halo in zip(chunks, halos):
        for r in range(0, end - start, 16):
            halo.wait(r)
            near = slice(halo.first + r, halo.first + r + 16)
            for c in range(0, cols, 128):
                across = slice(c, c + 128)
                e, o = ([ref[i, near, across] for i in range(RADIUS)] for ref in halo.refs)
                o = [jnp.where(edge, 0.0, v) for v in o]
                layers = [jnp.where(odd, a, b) for a, b in zip(e, o)]
                layers += [density[i, start + r : start + r + 16, across] for i in range(depth)]
                layers += [jnp.where(odd, b, a) for a, b in zip(e, o)]
                at = (slice(first + r, first + r + 16), across)
                for i, value in enumerate(along_z(layers, depth)):
                    halves[(0, i, *at)], halves[(1, i, *at)] = parts(value)
        first += end - start
    flat = halves[...].reshape(2 * depth * rows, cols)
    total = jnp.dot(flat, weights[...], preferred_element_type=jnp.float32)
    total = total.reshape(2, depth, rows, cols)
    out[...] = total[0] + total[1]


def scratch_zx(depth, cols, chunks):
    rows = sum(end - start for start, end in chunks)
    pieces = sum(-(-(end - start) // PIECE) for start, end in chunks)
    return [
        pltpu.VMEM((2, depth, rows, cols), jnp.bfloat16),
        pltpu.VMEM((2, RADIUS, rows, cols), jnp.float32),
        pltpu.SemaphoreType.DMA((pieces, 2)),
    ]


def fetch(chunks, refs, held, sems):
    halos, first, sem = [], 0, 0
    for n, (start, end) in enumerate(chunks):
        halos.append(Halo(refs[2 * n], refs[2 * n + 1], held, sems, first, sem))
        first, sem = first + end - start, halos[-1].sem
    return halos


def zx_kernel(chunks, place, density, weights, *refs):
    refs, (out, tail, head, halves, held, sems) = refs[:-6], refs[-6:]
    halos = fetch(chunks, refs, held, sems)
    filter_zx(density, chunks, halos, place, weights, out, halves)
    edge = chunks[0][1] - chunks[0][0]
    tail[...] = out[:, edge - REACH : edge, :]
    head[...] = out[:, edge : edge + REACH, :]


def coverage(index, whole):
    total = jnp.zeros(index.shape, jnp.float32)
    for offset in range(-RADIUS, RADIUS + 1):
        inside = (index + offset >= 0) & (index + offset < whole)
        total = total + jnp.where(inside, float(RADIUS + 1 - abs(offset)), 0.0)
    return total


def tally(t):
    ones = 1.0 - t * t
    return t.reshape(-1, 8, t.shape[1]).sum(0), ones.reshape(-1, 8, t.shape[1]).sum(0)


def band(rows):
    tall = rows + 2 * REACH
    column = lax.broadcasted_iota(jnp.int32, (rows, 2 * tall), 1)
    column = jnp.where(column >= tall, column - tall, column)
    away = jnp.abs(column - REACH - lax.broadcasted_iota(jnp.int32, (rows, 2 * tall), 0))
    return jnp.maximum(RADIUS + 1 - away, 0).astype(jnp.float32).astype(jnp.bfloat16)


def filter_y(pieces, start, kind, rz, scale, beta, field):
    depth, rows, cols = field.shape
    blocks = -(-rows // MOST)
    size = -(-rows // (8 * blocks)) * 8
    both = jnp.zeros((2, 8, cols), jnp.float32)
    for at in range(0, rows, size):
        length = min(size, rows - at)
        w = band(length)
        here = slice(start + at, start + at + length)
        for i in range(depth):
            tall = pieces(i, at, length + 2 * REACH)
            top, rest = parts(tall)
            stack = jnp.concatenate([top, rest], axis=0)
            smooth = jnp.dot(w, stack, preferred_element_type=jnp.float32)
            filtered = smooth * (scale[here, :] * rz[i])
            what = kind[i, here, :]
            value = jnp.where(what == 0, filtered, jnp.where(what == 2, FAR, -FAR))
            field[i, at : at + length, :] = value
            both += jnp.stack(tally(jnp.tanh(beta * (value - 0.5))))
    return both


def joined(*refs):
    def pieces(i, at, length):
        found, first = [], 0
        for ref, low, high in refs:
            a, b = max(at, first), min(at + length, first + high - low)
            if a < b:
                found.append(ref[i, low + a - first : low + b - first, :])
            first += high - low
        return found[0] if len(found) == 1 else jnp.concatenate(found, axis=0)

    return pieces


def left_kernel(edge, beta, _, before, a, kind, rz, scale, field, sums):
    one = joined((before, 0, REACH), (a, edge, a.shape[1]))
    sums[...] = filter_y(one, 0, kind, rz, scale, beta[0], field)


def right_kernel(
    edge, chunk, place, beta, density, even, odd, weights, a, after, kind, rz, scale, sums,
    own, field, more, halves, held, sems,
):
    halos = fetch((chunk,), (even, odd), held, sems)
    filter_zx(density, (chunk,), halos, place, weights, own, halves)
    one = joined((own, 0, own.shape[1]), (a, 0, edge), (after, 0, REACH))
    more[...] = sums[...] + filter_y(one, chunk[0] + REACH, kind, rz, scale, beta[0], field)


def middle_kernel(
    chunk, place, beta, density, even, odd, weights, a, b, kind, rz, scale, sums,
    field, message, own, halves,
):
    filter_zx(density, (chunk,), (Near(even, odd),), place, weights, own, halves)
    one = joined((a, a.shape[1] - 2 * REACH, a.shape[1]), (own, 0, own.shape[1]), (b, 0, 2 * REACH))
    both = filter_y(one, chunk[0] - REACH, kind, rz, scale, beta[0], field)
    pack(sums[...] + both, message)


def pack(both, message):
    folded = both[:, :, 0:128] + both[:, :, 128:256] + both[:, :, 256:384]
    row = jnp.sum(folded, axis=1)
    row = row[:, 0:64] + row[:, 64:128]
    line = jnp.concatenate([row[0:1], row[1:2]], axis=1)
    message[...] = jnp.broadcast_to(line, message.shape)


def newton(cells, message, level, beta, fraction):
    line = jnp.sum(message[...], axis=0, keepdims=True)
    lane = lax.broadcasted_iota(jnp.int32, line.shape, 1)
    total = jnp.sum(jnp.where(lane < 64, line, 0.0), axis=1, keepdims=True)
    bends = jnp.sum(jnp.where(lane < 64, 0.0, line), axis=1, keepdims=True)
    volume = 0.5 * (cells + total)
    step = (volume - fraction[0] * cells) / (cells + 0.5 * beta[0] * bends)
    return level[...] + jnp.broadcast_to(step, level.shape)


def again_kernel(cells, count, message, level, beta, fraction, *refs):
    fields, (sent, moved) = refs[:count], refs[count:]
    eta = newton(cells, message, level, beta, fraction)
    moved[...] = eta
    b = beta[0]
    cols = fields[0].shape[2]
    eta = jnp.tile(eta[:1], (1, cols // 128))
    both = jnp.zeros((2, 8, cols), jnp.float32)
    for field in fields:
        for i in range(field.shape[0]):
            both += jnp.stack(tally(jnp.tanh(b * (field[i] - eta))))
    pack(both, sent)


def last_kernel(cells, count, message, level, beta, fraction, *refs):
    fields, (out, moved, held, sems) = refs[:count], refs[count:]
    eta = newton(cells, message, level, beta, fraction)
    moved[0] = eta[0, 0]
    b = beta[0]
    eta = jnp.tile(eta[:1], (1, held.shape[2] // 128))
    copies = []
    for i in range(held.shape[0]):
        first = 0
        for k, field in enumerate(fields):
            rows = pl.ds(first, field.shape[1])
            first += field.shape[1]
            held[i, rows, :] = 0.5 * (1.0 + jnp.tanh(b * (field[i] - eta)))
            at = (i, rows, slice(None))
            copies.append(pltpu.make_async_copy(held.at[at], out.at[at], sems.at[i * count + k]))
            copies[-1].start()
    for copy in copies:
        copy.wait()


def local(slabs, pencils, density, cell_kind, beta, fraction):
    depth, rows, cols = density.shape
    members = slabs * pencils
    cells = float(depth * slabs * rows * pencils * cols)
    pairs = [
        [
            (a, b)
            for i in range(k, slabs, 2)
            for a, b in ((i, (i + 1) % slabs), ((i + 1) % slabs, i))
        ]
        for k in (0, 1)
    ]
    parity = lax.axis_index("slab") % 2
    side = [(i, i + 1) for i in range(pencils - 1)]
    f32 = jnp.float32

    halos = []
    source = density
    for n, (start, end) in enumerate(CHUNKS):
        for k in (0, 1):
            first = jnp.where(parity == k, depth - RADIUS, 0)
            part = lax.dynamic_slice_in_dim(source[:, start:end], first, RADIUS, axis=0)
            halos.append(lax.ppermute(part, "slab", pairs[k]))
        if n == 0:
            source = lax.optimization_barrier(density)
    index = lax.axis_index("slab")
    place = jnp.stack([parity, ((index == 0) | (index == slabs - 1)).astype(jnp.int32)])

    near = lax.broadcasted_iota(jnp.int32, (cols, cols), 0)
    near = jnp.abs(near - lax.broadcasted_iota(jnp.int32, (cols, cols), 1))
    wx = jnp.maximum(RADIUS + 1 - near, 0).astype(jnp.bfloat16)
    rz = 1.0 / coverage(lax.axis_index("slab") * depth + jnp.arange(depth), depth * slabs)
    cy = coverage(lax.axis_index("pencil") * rows + jnp.arange(rows), rows * pencils)
    scale = 1.0 / (cy[:, None] * coverage(jnp.arange(cols), cols)[None, :])

    field = lambda n: jax.ShapeDtypeStruct((depth, n, cols), f32)
    sums = jax.ShapeDtypeStruct((2, 8, cols), f32)
    sent = jax.ShapeDtypeStruct((members, 128), f32)
    one = jax.ShapeDtypeStruct((1,), f32)
    anywhere = pl.BlockSpec(memory_space=pl.ANY)
    size_a = sum(end - start for start, end in CHUNKS[:2])
    edge = CHUNKS[0][1] - CHUNKS[0][0]
    mid, end = CHUNKS[3]
    smooth_a, tail, head = call(
        functools.partial(zx_kernel, CHUNKS[:2]), (field(size_a), field(REACH), field(REACH)),
        (place, density, wx, *halos[:4]), (VMEM,) * 3, [SMEM, VMEM, VMEM, *[anywhere] * 4],
        scratch_zx(depth, cols, CHUNKS[:2]), flops=20_000_000, moved=8_000_000,
    )
    before = lax.ppermute(tail, "pencil", side)
    after = lax.ppermute(head, "pencil", [(j, i) for i, j in side])
    field_a, sums_a = call(
        functools.partial(left_kernel, edge), (field(mid - REACH), sums),
        (beta, fraction, before, smooth_a, cell_kind, rz, scale),
        (VMEM,) * 2, [SMEM, SMEM, *[VMEM] * 3, SMEM, VMEM], flops=10_000_000, moved=4_000_000,
    )
    smooth_b, field_b, sums_b = call(
        functools.partial(right_kernel, edge, CHUNKS[2]),
        (field(CHUNKS[2][1] - end), field(rows - end - REACH), sums),
        (place, beta, density, *halos[4:6], wx, smooth_a, after, cell_kind, rz, scale, sums_a),
        (VMEM,) * 3,
        [SMEM, SMEM, VMEM, anywhere, anywhere, *[VMEM] * 4, SMEM, VMEM, VMEM],
        scratch_zx(depth, cols, CHUNKS[2:3]), flops=20_000_000, moved=8_000_000,
    )
    field_c, message = call(
        functools.partial(middle_kernel, CHUNKS[3]),
        (field(end - mid + 2 * REACH), sent),
        (place, beta, density, *halos[6:], wx, smooth_a, smooth_b, cell_kind, rz, scale, sums_b),
        (VMEM,) * 2, [SMEM, SMEM, *[VMEM] * 7, SMEM, VMEM, VMEM],
        [pltpu.VMEM((depth, end - mid, cols), f32), scratch_zx(depth, cols, CHUNKS[3:])[0]],
        flops=6_000_000, moved=3_000_000,
    )
    fields = [field_a, field_c, field_b]
    count = len(fields)
    level = jnp.full((8, 128), 0.5, f32)
    scalars = [VMEM, VMEM, SMEM, SMEM]
    for step in range(ITERS):
        message = lax.all_to_all(message, DEVICES, 0, 0, tiled=True)
        ins = [message, level, beta, fraction, *fields]
        if step < ITERS - 1:
            message, level = call(
                functools.partial(again_kernel, cells, count),
                (sent, jax.ShapeDtypeStruct(level.shape, f32)), ins,
                (VMEM, VMEM), scalars + [VMEM] * count, flops=6_000_000, moved=3_600_000,
            )
    return call(
        functools.partial(last_kernel, cells, count), (field(rows), one), ins,
        (pl.BlockSpec(memory_space=pl.ANY), SMEM), scalars + [VMEM] * count,
        [pltpu.VMEM(density.shape, f32), pltpu.SemaphoreType.DMA((count * depth,))],
        flops=6_000_000, moved=7_200_000,
    )


def solution(mesh):
    P = jax.sharding.PartitionSpec
    grid = P("slab", "pencil", None)
    return jax.shard_map(
        functools.partial(local, mesh.shape["slab"], mesh.shape["pencil"]),
        mesh=mesh,
        in_specs=(grid, grid, P(), P()),
        out_specs=(grid, P()),
        check_vma=False,
    )
```
